8 devices in a mesh: fsdp: 8 (over z, y, x, core).
Axes of the slice: x: 2, y: 2, z: 1, core: 2. Of those that a mesh axis runs over, the one named last changes fastest.
Arguments:
- hidden: bfloat16 [6, 8192, 576], P(None, 'fsdp')
- w_gate: bfloat16 [6, 576, 1536], P(None, 'fsdp')
- w_up: bfloat16 [6, 576, 1536], P(None, 'fsdp')
- w_down: bfloat16 [6, 1536, 576], P(None, 'fsdp')
- w_out: bfloat16 [576, 49152], P('fsdp')
- targets: int32 [8192], P('fsdp')
- loss_mask: int32 [8192], P('fsdp')
Outputs:
- output 1: float32 [6, 576, 1536], P(None, 'fsdp')
- output 2: float32 [6, 576, 1536], P(None, 'fsdp')
- output 3: float32 [6, 1536, 576], P(None, 'fsdp')
- output 4: float32 [576, 49152], P('fsdp')
- output 5: bfloat16 [8192, 576], P('fsdp')
- output 6: float32 [], replicated
All inputs are finite; a program needn't handle non-finite values.
Results may differ from the reference program's by a relative error of at most 0.0151241.
Values are sent between devices in bfloat16 or wider.
A program may use at most 1 GiB of HBM per device.

```python
import jax
import jax.numpy as jnp
from jax import lax

LAYERS = 6
TOK_DEV = 1024
GROUP_SIZE = 8
HIDDEN = 576
FFN_DIM = 1536
VOCAB_SIZE = 49152
TOKENS = 8192

NORM_EPS = 1e-5


def draw_labels(label_key):
    key_tgt, key_rate, key_keep = jax.random.split(label_key, 3)
    targets = jax.random.randint(key_tgt, (TOKENS,), 0, VOCAB_SIZE, dtype=jnp.int32)
    targets = targets.at[0].set(VOCAB_SIZE - 1)
    keep_rate = jax.random.randint(key_rate, (GROUP_SIZE, 1), 2, 17, dtype=jnp.int32)
    ticket = jax.random.randint(key_keep, (GROUP_SIZE, TOK_DEV), 0, 16, dtype=jnp.int32)
    loss_mask = (ticket < keep_rate).astype(jnp.int32).reshape(TOKENS)
    loss_mask = loss_mask.at[0].set(1)
    return targets, loss_mask


def setup_inputs(seed: int = 0) -> dict:
    sub_keys = jax.random.split(jax.random.key(seed), 6)
    hidden = jax.random.normal(sub_keys[0], (LAYERS, TOKENS, HIDDEN), jnp.float32).astype(jnp.bfloat16)
    w_gate = (jax.random.normal(sub_keys[1], (LAYERS, HIDDEN, FFN_DIM), jnp.float32) * HIDDEN ** -0.5).astype(jnp.bfloat16)
    w_up = (jax.random.normal(sub_keys[2], (LAYERS, HIDDEN, FFN_DIM), jnp.float32) * HIDDEN ** -0.5).astype(jnp.bfloat16)
    w_down = (jax.random.normal(sub_keys[3], (LAYERS, FFN_DIM, HIDDEN), jnp.float32) * FFN_DIM ** -0.5).astype(jnp.bfloat16)
    w_out = (jax.random.normal(sub_keys[4], (HIDDEN, VOCAB_SIZE), jnp.float32) * HIDDEN ** -0.5).astype(jnp.bfloat16)
    targets, loss_mask = draw_labels(sub_keys[5])
    return {'hidden': hidden, 'w_gate': w_gate, 'w_up': w_up, 'w_down': w_down, 'w_out': w_out, 'targets': targets, 'loss_mask': loss_mask}


def norm_apply(x_in):
    x_f32 = x_in.astype(jnp.float32)
    inv_rms = lax.rsqrt(jnp.mean(x_f32 * x_f32, axis=-1, keepdims=True) + NORM_EPS)
    return (x_f32 * inv_rms).astype(jnp.bfloat16)


def norm_grad(x_in, grad_y):
    x_f32 = x_in.astype(jnp.float32)
    inv_rms = lax.rsqrt(jnp.mean(x_f32 * x_f32, axis=-1, keepdims=True) + NORM_EPS)
    x_dot_grad = jnp.mean(x_f32 * grad_y, axis=-1, keepdims=True)
    return inv_rms * grad_y - x_f32 * (inv_rms * inv_rms * inv_rms) * x_dot_grad


def block_forward(h_in, gate_w, up_w):
    normed = norm_apply(h_in)
    gate_pre = jnp.dot(normed, gate_w, preferred_element_type=jnp.float32)
    up_pre = jnp.dot(normed, up_w, preferred_element_type=jnp.float32)
    gate_sig = jax.nn.sigmoid(gate_pre)
    gated_act = (gate_pre * gate_sig * up_pre).astype(jnp.bfloat16)
    return normed, gate_pre, up_pre, gate_sig, gated_act


def block_backward(h_in, grad_in, gate_w, up_w, down_w, saved_fwd):
    normed, gate_pre, up_pre, gate_sig, gated_act = saved_fwd
    grad_bf16 = grad_in.astype(jnp.bfloat16)
    grad_act = jnp.dot(grad_bf16, down_w.T, preferred_element_type=jnp.float32)
    grad_gate_pre = (grad_act * up_pre * gate_sig * (1.0 + gate_pre * (1.0 - gate_sig))).astype(jnp.bfloat16)
    grad_up_pre = (grad_act * gate_pre * gate_sig).astype(jnp.bfloat16)
    grad_down_w = jnp.dot(gated_act.T, grad_bf16, preferred_element_type=jnp.float32)
    grad_gate_w = jnp.dot(normed.T, grad_gate_pre, preferred_element_type=jnp.float32)
    grad_up_w = jnp.dot(normed.T, grad_up_pre, preferred_element_type=jnp.float32)
    grad_norm = jnp.dot(grad_gate_pre, gate_w.T, preferred_element_type=jnp.float32) + jnp.dot(grad_up_pre, up_w.T, preferred_element_type=jnp.float32)
    return grad_in + norm_grad(h_in, grad_norm), grad_gate_w, grad_up_w, grad_down_w


def head_grads(h_top, out_w, tgt_ids, mask_ids, mask_count):
    normed_top = norm_apply(h_top)
    logits = jnp.dot(normed_top, out_w, preferred_element_type=jnp.float32)
    shifted = logits - jnp.max(logits, axis=-1, keepdims=True)
    exp_shift = jnp.exp(shifted)
    exp_sum = jnp.sum(exp_shift, axis=-1, keepdims=True)
    is_target = lax.broadcasted_iota(jnp.int32, (1, logits.shape[1]), 1) == tgt_ids[:, None]
    tok_loss = jnp.log(exp_sum[:, 0]) - jnp.sum(jnp.where(is_target, shifted, 0.0), axis=-1)
    weight = mask_ids.astype(jnp.float32) / mask_count
    loss_part = jnp.sum(weight * tok_loss)
    grad_logits = (weight[:, None] * (exp_shift / exp_sum - is_target.astype(jnp.float32))).astype(jnp.bfloat16)
    grad_wout = jnp.dot(normed_top.T, grad_logits, preferred_element_type=jnp.float32)
    grad_top = norm_grad(h_top, jnp.dot(grad_logits, out_w.T, preferred_element_type=jnp.float32))
    return loss_part, grad_wout, grad_top


def reference(hidden, w_gate, w_up, w_down, w_out, targets, loss_mask):
    top_layer = LAYERS - 1
    hidden_blocks = hidden.reshape(LAYERS, GROUP_SIZE, TOK_DEV, HIDDEN)
    mask_count = jnp.sum(loss_mask).astype(jnp.float32)

    def head_step(carry_sums, block_in):
        h_block, tgt_block, mask_block = block_in
        saved_fwd = block_forward(h_block, w_gate[top_layer], w_up[top_layer])
        h_top = (h_block.astype(jnp.float32) + jnp.dot(saved_fwd[4], w_down[top_layer], preferred_element_type=jnp.float32)).astype(jnp.bfloat16)
        loss_part, grad_wout, grad_top = head_grads(h_top, w_out, tgt_block, mask_block, mask_count)
        return (carry_sums[0] + loss_part, carry_sums[1] + grad_wout), grad_top

    head_init = (jnp.zeros((), jnp.float32), jnp.zeros((HIDDEN, VOCAB_SIZE), jnp.float32))
    (mean_loss, grad_out), grad_top = lax.scan(head_step, head_init, (hidden_blocks[top_layer], targets.reshape(GROUP_SIZE, TOK_DEV), loss_mask.reshape(GROUP_SIZE, TOK_DEV)))

    def layer_step(grad_run, layer_in):
        h_layer, gate_w, up_w, down_w = layer_in

        def block_step(carry_sums, block_in):
            h_block, grad_block = block_in
            saved_fwd = block_forward(h_block, gate_w, up_w)
            grad_next, grad_gate_w, grad_up_w, grad_down_w = block_backward(h_block, grad_block, gate_w, up_w, down_w, saved_fwd)
            return (carry_sums[0] + grad_gate_w, carry_sums[1] + grad_up_w, carry_sums[2] + grad_down_w), grad_next

        zero_sums = (jnp.zeros((HIDDEN, FFN_DIM), jnp.float32), jnp.zeros((HIDDEN, FFN_DIM), jnp.float32), jnp.zeros((FFN_DIM, HIDDEN), jnp.float32))
        layer_sums, grad_prev = lax.scan(block_step, zero_sums, (h_layer, grad_run))
        return grad_prev, layer_sums

    grad_first, (grad_gate, grad_up, grad_down) = lax.scan(layer_step, grad_top, (hidden_blocks, w_gate, w_up, w_down), reverse=True)
    grad_hidden = grad_first.reshape(TOKENS, HIDDEN).astype(jnp.bfloat16)
    return grad_gate, grad_up, grad_down, grad_out, grad_hidden, mean_loss
```

```python
import functools

import jax
import jax.numpy as jnp
from jax import lax
from jax.experimental import pallas as pl
from jax.experimental.pallas import tpu as pltpu
from jax.sharding import PartitionSpec as P

NORM_EPS = 1e-5
AXIS = 'fsdp'
NDEV = 8
F32 = jnp.float32
BF16 = jnp.bfloat16
VMEM_LIMIT = 60 * 1024 * 1024
VMEM_MAX = 67043328


def params(*sem, **kw):
    return pltpu.CompilerParams(dimension_semantics=sem or None, vmem_limit_bytes=VMEM_LIMIT, **kw)


def contract_cols(left, right):
    return lax.dot_general(left, right, (((1,), (1,)), ((), ())), preferred_element_type=F32)


def contract_rows(left, right):
    return lax.dot_general(left, right, (((0,), (0,)), ((), ())), preferred_element_type=F32)


def dot(left, right):
    return jnp.dot(left, right, preferred_element_type=F32)


def inv_rms_of(x_f32):
    return lax.rsqrt(jnp.mean(x_f32 * x_f32, axis=-1, keepdims=True) + NORM_EPS)


def norm_grad(x_f32, grad_y):
    r = inv_rms_of(x_f32)
    m = jnp.mean(x_f32 * grad_y, axis=-1, keepdims=True)
    return r * grad_y - x_f32 * (r * r * r) * m


def small_gather_kernel(x_ref, o_ref, send_sem, recv_sem):
    me = lax.axis_index(AXIS)
    barrier = pltpu.get_barrier_semaphore()
    for k in range(1, NDEV):
        pl.semaphore_signal(barrier, inc=1, device_id=(jnp.bitwise_xor(me, k),), device_id_type=pl.DeviceIdType.MESH)
    pl.semaphore_wait(barrier, NDEV - 1)
    copies = []
    for k in range(1, NDEV):
        copies.append(pltpu.make_async_remote_copy(
            src_ref=x_ref, dst_ref=o_ref.at[k], send_sem=send_sem.at[k], recv_sem=recv_sem.at[k],
            device_id=(jnp.bitwise_xor(me, k),), device_id_type=pl.DeviceIdType.MESH))
    for c in copies:
        c.start()
    o_ref[0] = x_ref[...]
    for c in copies:
        c.wait()


def small_gather(x, cid):
    return pl.pallas_call(
        small_gather_kernel,
        out_shape=jax.ShapeDtypeStruct((NDEV,) + x.shape, x.dtype),
        in_specs=[pl.BlockSpec(memory_space=pltpu.VMEM)],
        out_specs=pl.BlockSpec(memory_space=pltpu.VMEM),
        scratch_shapes=[pltpu.SemaphoreType.DMA((NDEV,)), pltpu.SemaphoreType.DMA((NDEV,))],
        compiler_params=pltpu.CompilerParams(collective_id=cid, has_side_effects=True),
        name=f'small_gather_{cid}',
    )(x)


def top_forward_kernel(h_ref, wg_ref, wu_ref, wd_ref, t_ref, z_ref, n_sc, acc_sc):
    f = pl.program_id(0)

    @pl.when(f == 0)
    def _():
        h = h_ref[...].astype(F32)
        n_sc[...] = (h * inv_rms_of(h)).astype(BF16)
        acc_sc[...] = h

    n = n_sc[...]
    u = dot(n, wg_ref[...])
    v = dot(n, wu_ref[...])
    a = (u * jax.nn.sigmoid(u) * v).astype(BF16)
    acc_sc[...] += dot(a, wd_ref[...])

    @pl.when(f == pl.num_programs(0) - 1)
    def _():
        t = acc_sc[...].astype(BF16)
        t_ref[...] = t
        tf = t.astype(F32)
        z_ref[...] = (tf * inv_rms_of(tf)).astype(BF16)


def top_forward(hidden, layer, wg, wu, wd, wl, chunk=512):
    tok, width = hidden.shape[1:]
    inner = wg.shape[2]
    return pl.pallas_call(
        top_forward_kernel,
        grid=(inner // chunk,),
        out_shape=(jax.ShapeDtypeStruct((tok, width), BF16),) * 2,
        in_specs=[
            pl.BlockSpec((None, tok, width), lambda f: (layer, 0, 0)),
            pl.BlockSpec((None, width, chunk), lambda f: (wl, 0, f)),
            pl.BlockSpec((None, width, chunk), lambda f: (wl, 0, f)),
            pl.BlockSpec((None, chunk, width), lambda f: (wl, f, 0)),
        ],
        out_specs=(pl.BlockSpec((tok, width), lambda f: (0, 0)),) * 2,
        scratch_shapes=[pltpu.VMEM((tok, width), BF16), pltpu.VMEM((tok, width), F32)],
        compiler_params=params('arbitrary'),
        cost_estimate=pl.CostEstimate(flops=6 * tok * width * inner, bytes_accessed=10**7, transcendentals=0),
        name='top_forward',
    )(hidden, wg, wu, wd)


def remote(src, dst, send_sem, recv_sem, dev):
    return pltpu.make_async_remote_copy(src_ref=src, dst_ref=dst, send_sem=send_sem, recv_sem=recv_sem,
                                        device_id=(dev,), device_id_type=pl.DeviceIdType.MESH)


def blocks_kernel(h_ref, g0_ref, wgt_ref, wut_ref, wdt_ref, wg_ref, wu_ref, wd_ref,
                  og_ref, ou_ref, od_ref, gh_ref,
                  n_sc, k_sc, dn_sc, g_sc, keep_w, keep_d, give_w, give_d, got_w, got_d,
                  out_w, out_d, in_w, in_d, own_w, own_d,
                  g0_sem, s1_send, s1_recv, s3_send, s3_recv, *, layers, nf):
    step = pl.program_id(0)
    compute_steps = layers * nf
    g = jnp.where(step < compute_steps, step // nf, step - compute_steps + layers)
    f = jnp.where(step < compute_steps, step % nf, 0)
    me = lax.axis_index(AXIS)
    chip, core = me // 2, me % 2
    rows_w = keep_w.shape[2]
    rows_d = keep_d.shape[1]
    chunk = wg_ref.shape[1]

    def stage1(layer):
        slot = layer % 2
        mate = chip * 2 + 1 - core
        return (remote(give_w, got_w.at[slot], s1_send.at[0], s1_recv.at[slot, 0], mate),
                remote(give_d, got_d.at[slot], s1_send.at[1], s1_recv.at[slot, 1], mate))

    def stage3(layer):
        slot = layer % 2
        copies = []
        for k in (1, 2, 3):
            dev = jnp.bitwise_xor(me, 2 * k)
            copies.append(remote(out_w.at[k - 1], in_w.at[slot, k - 1], s3_send.at[k - 1, 0], s3_recv.at[slot, k - 1, 0], dev))
            copies.append(remote(out_d.at[k - 1], in_d.at[slot, k - 1], s3_send.at[k - 1, 1], s3_recv.at[slot, k - 1, 1], dev))
        return copies

    @pl.when(step == 0)
    def _():
        cp = pltpu.make_async_copy(g0_ref, g_sc, g0_sem)
        cp.start()
        barrier = pltpu.get_barrier_semaphore()
        for k in (1, 2, 4, 6):
            pl.semaphore_signal(barrier, inc=1, device_id=(jnp.bitwise_xor(me, k),), device_id_type=pl.DeviceIdType.MESH)
        pl.semaphore_wait(barrier, 4)
        cp.wait()

    @pl.when((f == 0) & (g >= 2))
    def _():
        layer = layers + 1 - g
        slot = layer % 2
        for cp in stage3(layer):
            cp.wait()
        for x, o_ref in ((0, og_ref), (1, ou_ref)):
            o_ref[...] = (own_w[x] + in_w[slot, 0, x].astype(F32)
                          + (in_w[slot, 1, x].astype(F32) + in_w[slot, 2, x].astype(F32)))
        od_ref[...] = own_d[...] + in_d[slot, 0].astype(F32) + (in_d[slot, 1].astype(F32) + in_d[slot, 2].astype(F32))

    @pl.when((f == 0) & (g >= 1) & (g <= layers))
    def _():
        layer = layers - g
        slot = layer % 2
        for cp in stage1(layer):
            cp.wait()
        copies = stage3(layer)
        for k in (3, 1, 2):
            q = jnp.bitwise_xor(chip, k)
            for x in (0, 1):
                out_w[k - 1, x] = (keep_w[x, q] + got_w[slot, x, q].astype(F32)).astype(BF16)
            out_d[k - 1] = (keep_d[q] + got_d[slot, q].astype(F32)).astype(BF16)
            copies[2 * k - 2].start()
            copies[2 * k - 1].start()
        for x in (0, 1):
            own_w[x] = keep_w[x, chip] + got_w[slot, x, chip].astype(F32)
        own_d[...] = keep_d[chip] + got_d[slot, chip].astype(F32)

    @pl.when(step < compute_steps)
    def _():
        @pl.when(f == 0)
        def _():
            h = h_ref[...].astype(F32)
            n_sc[...] = (h * inv_rms_of(h)).astype(BF16)
            k_sc[...] = g_sc[...].astype(BF16)

        is_top = g == 0
        wg = jnp.where(is_top, wgt_ref[...], wg_ref[...])
        wu = jnp.where(is_top, wut_ref[...], wu_ref[...])
        wd = jnp.where(is_top, wdt_ref[...], wd_ref[...])
        n = n_sc[...]
        k = k_sc[...]
        u = dot(n, wg)
        v = dot(n, wu)
        e = contract_cols(k, wd)
        s = jax.nn.sigmoid(u)
        us = u * s
        a = (us * v).astype(BF16)
        du = (e * v * s * (1.0 + u * (1.0 - s))).astype(BF16)
        dv = (e * us).astype(BF16)
        gd = contract_rows(a, k)
        even = core == 0
        for c in range(chunk // (2 * rows_d)):
            lo = gd[2 * c * rows_d:(2 * c + 1) * rows_d]
            hi = gd[(2 * c + 1) * rows_d:(2 * c + 2) * rows_d]
            q = f * (chunk // (2 * rows_d)) + c
            keep_d[q] = jnp.where(even, lo, hi)
            give_d[q] = jnp.where(even, hi, lo).astype(BF16)
        cols = pl.ds(pl.multiple_of(f * chunk, chunk), chunk)
        for x, d in ((0, du), (1, dv)):
            gw = contract_rows(n, d)
            for q in range(4):
                lo = gw[2 * q * rows_w:(2 * q + 1) * rows_w]
                hi = gw[(2 * q + 1) * rows_w:(2 * q + 2) * rows_w]
                keep_w[x, q, :, cols] = jnp.where(even, lo, hi)
                give_w[x, q, :, cols] = jnp.where(even, hi, lo).astype(BF16)
        dn = contract_cols(du, wg) + contract_cols(dv, wu)

        @pl.when(f == 0)
        def _():
            dn_sc[...] = dn

        @pl.when(f > 0)
        def _():
            dn_sc[...] += dn

        @pl.when(f == nf - 1)
        def _():
            for cp in stage1(layers - 1 - g):
                cp.start()
            h = h_ref[...].astype(F32)
            g_new = g_sc[...] + norm_grad(h, dn_sc[...])
            g_sc[...] = g_new
            gh_ref[...] = g_new.astype(BF16)


def blocks_backward(hidden, g0, top_w, rest_w, chunk=384):
    layers, tok, width = hidden.shape
    inner = top_w[0].shape[2]
    nf = inner // chunk
    rw, rd = width // NDEV, inner // NDEV
    last = layers * nf

    def layer_of(s):
        return jnp.maximum(layers - 1 - s // nf, 0)

    def chunk_of(s):
        return jnp.where(s < last, s % nf, nf - 1)

    def rest_of(s):
        return jnp.minimum(layer_of(s), layers - 2)

    def top_chunk(s):
        return jnp.minimum(s, nf - 1)

    def out_of(s):
        gg = jnp.where(s < last, s // nf, s - last + layers)
        return jnp.minimum(layers + 1 - gg, layers - 1)

    return pl.pallas_call(
        functools.partial(blocks_kernel, layers=layers, nf=nf),
        grid=(last + 2,),
        out_shape=(
            jax.ShapeDtypeStruct((layers, rw, inner), F32),
            jax.ShapeDtypeStruct((layers, rw, inner), F32),
            jax.ShapeDtypeStruct((layers, rd, width), F32),
            jax.ShapeDtypeStruct((tok, width), BF16),
        ),
        in_specs=[
            pl.BlockSpec((None, tok, width), lambda s: (layer_of(s), 0, 0)),
            pl.BlockSpec(memory_space=pl.ANY),
            pl.BlockSpec((None, width, chunk), lambda s: (0, 0, top_chunk(s))),
            pl.BlockSpec((None, width, chunk), lambda s: (0, 0, top_chunk(s))),
            pl.BlockSpec((None, chunk, width), lambda s: (0, top_chunk(s), 0)),
            pl.BlockSpec((None, width, chunk), lambda s: (rest_of(s), 0, chunk_of(s))),
            pl.BlockSpec((None, width, chunk), lambda s: (rest_of(s), 0, chunk_of(s))),
            pl.BlockSpec((None, chunk, width), lambda s: (rest_of(s), chunk_of(s), 0)),
        ],
        out_specs=(
            pl.BlockSpec((None, rw, inner), lambda s: (out_of(s), 0, 0)),
            pl.BlockSpec((None, rw, inner), lambda s: (out_of(s), 0, 0)),
            pl.BlockSpec((None, rd, width), lambda s: (out_of(s), 0, 0)),
            pl.BlockSpec((tok, width), lambda s: (0, 0)),
        ),
        scratch_shapes=[
            pltpu.VMEM((tok, width), BF16), pltpu.VMEM((tok, width), BF16),
            pltpu.VMEM((tok, width), F32), pltpu.VMEM((tok, width), F32),
            pltpu.VMEM((2, 4, rw, inner), F32), pltpu.VMEM((4, rd, width), F32),
            pltpu.VMEM((2, 4, rw, inner), BF16), pltpu.VMEM((4, rd, width), BF16),
            pltpu.VMEM((2, 2, 4, rw, inner), BF16), pltpu.VMEM((2, 4, rd, width), BF16),
            pltpu.VMEM((3, 2, rw, inner), BF16), pltpu.VMEM((3, rd, width), BF16),
            pltpu.VMEM((2, 3, 2, rw, inner), BF16), pltpu.VMEM((2, 3, rd, width), BF16),
            pltpu.VMEM((2, rw, inner), F32), pltpu.VMEM((rd, width), F32),
            pltpu.SemaphoreType.DMA,
            pltpu.SemaphoreType.DMA((2,)), pltpu.SemaphoreType.DMA((2, 2)),
            pltpu.SemaphoreType.DMA((3, 2)), pltpu.SemaphoreType.DMA((2, 3, 2)),
        ],
        compiler_params=pltpu.CompilerParams(dimension_semantics=('arbitrary',), vmem_limit_bytes=VMEM_MAX,
                                             collective_id=3, has_side_effects=True),
        cost_estimate=pl.CostEstimate(flops=layers * 16 * tok * width * inner, bytes_accessed=2 * 10**7, transcendentals=0),
        name='blocks_backward',
    )(hidden, g0, *top_w, *rest_w)


def spread(row_ref, dst):
    for r in range(row_ref.shape[0]):
        dst[r * 128:(r + 1) * 128, :] = jnp.broadcast_to(row_ref[r:r + 1, :], (128, 128)).T


def gather_up(col):
    rows = [col[r * 128:(r + 1) * 128, :].T[0:1, :] for r in range(col.shape[0] // 128)]
    return jnp.concatenate(rows, axis=0)


def pass1_kernel(z_ref, w_ref, tgt_ref, l_ref, st_ref, m_sc, s_sc, t_sc, tgt_sc, *, chunk, sub, vocab_local):
    j = pl.program_id(1)
    base = lax.axis_index(AXIS) * vocab_local + j * chunk

    @pl.when(j == 0)
    def _():
        m_sc[...] = jnp.full_like(m_sc, -jnp.inf)
        s_sc[...] = jnp.zeros_like(s_sc)
        t_sc[...] = jnp.zeros_like(t_sc)
        spread(tgt_ref, tgt_sc)

    z = z_ref[...]
    lane = lax.broadcasted_iota(jnp.int32, (1, 128), 1)
    for c in range(chunk // sub):
        l = dot(z, w_ref[:, pl.ds(pl.multiple_of(j * chunk, chunk) + c * sub, sub)])
        l_ref[:, c * sub:(c + 1) * sub] = l
        groups = [l[:, x * 128:(x + 1) * 128] for x in range(sub // 128)]
        m_old = m_sc[...]
        m_new = m_old
        for gr in groups:
            m_new = jnp.maximum(m_new, gr)
        s = s_sc[...] * jnp.exp(m_old - m_new)
        t = t_sc[...]
        tgt = tgt_sc[...] - (base + c * sub) - lane
        for x, gr in enumerate(groups):
            s = s + jnp.exp(gr - m_new)
            t = t + jnp.where(tgt == x * 128, gr, 0.0)
        m_sc[...] = m_new
        s_sc[...] = s
        t_sc[...] = t

    @pl.when(j == pl.num_programs(1) - 1)
    def _():
        m = m_sc[...]
        row_m = jnp.max(m, axis=1, keepdims=True)
        row_s = jnp.sum(s_sc[...] * jnp.exp(m - row_m), axis=1, keepdims=True)
        lse = row_m + jnp.log(row_s)
        t = jnp.sum(t_sc[...], axis=1, keepdims=True)
        shape = m.shape
        st_ref[0] = gather_up(jnp.broadcast_to(lse, shape))
        st_ref[1] = gather_up(jnp.broadcast_to(t, shape))


def pass1(z_all, w_loc, tgt_rows, chunk=1024, sub=512, tile=1024):
    tokens, width = z_all.shape
    vl = w_loc.shape[1]
    return pl.pallas_call(
        functools.partial(pass1_kernel, chunk=chunk, sub=sub, vocab_local=vl),
        grid=(tokens // tile, vl // chunk),
        out_shape=(jax.ShapeDtypeStruct((tokens, vl), F32), jax.ShapeDtypeStruct((2, tokens // 128, 128), F32)),
        in_specs=[
            pl.BlockSpec((tile, width), lambda i, j: (i, 0)),
            pl.BlockSpec((width, vl), lambda i, j: (0, 0)),
            pl.BlockSpec((tile // 128, 128), lambda i, j: (i, 0)),
        ],
        out_specs=(
            pl.BlockSpec((tile, chunk), lambda i, j: (i, j)),
            pl.BlockSpec((2, tile // 128, 128), lambda i, j: (0, i, 0)),
        ),
        scratch_shapes=[pltpu.VMEM((tile, 128), F32)] * 3 + [pltpu.VMEM((tile, 128), jnp.int32)],
        compiler_params=params('arbitrary', 'arbitrary'),
        cost_estimate=pl.CostEstimate(flops=2 * tokens * width * vl, bytes_accessed=4 * tokens * vl, transcendentals=tokens * vl),
        name='head_pass1',
    )(z_all, w_loc, tgt_rows)


def pass2_kernel(*refs, chunk, sub, vocab_local, part_base, first):
    if first:
        l_ref, z_ref, w_ref, lse_ref, wt_ref, tgt_ref, gw_ref, dz_ref, zt_sc, q_sc, lse_sc, wt_sc, tgt_sc = refs
        dzi_ref = None
    else:
        l_ref, z_ref, w_ref, lse_ref, wt_ref, tgt_ref, dzi_ref, gw_ref, dz_ref, zt_sc, q_sc, lse_sc, wt_sc, tgt_sc = refs
    i, j = pl.program_id(0), pl.program_id(1)
    base = lax.axis_index(AXIS) * vocab_local + part_base + j * chunk

    @pl.when(j == 0)
    def _():
        spread(lse_ref, lse_sc)
        spread(wt_ref, wt_sc)
        spread(tgt_ref, tgt_sc)
        zt_sc[...] = z_ref[...].T
        dz_ref[...] = jnp.zeros_like(dz_ref) if first else dzi_ref[...]

    @pl.when((i == 0) & (j == 0))
    def _():
        gw_ref[...] = jnp.zeros_like(gw_ref)

    lane = lax.broadcasted_iota(jnp.int32, (1, 128), 1)
    zt = zt_sc[...]
    for c in range(chunk // sub):
        lse = lse_sc[...]
        wt = wt_sc[...]
        tgt = tgt_sc[...] - (base + c * sub) - lane
        for x in range(sub // 128):
            lo = c * sub + x * 128
            p = jnp.exp(l_ref[:, lo:lo + 128] - lse)
            q_sc[:, lo:lo + 128] = (wt * (p - jnp.where(tgt == x * 128, 1.0, 0.0))).astype(BF16)
        cols = pl.ds(pl.multiple_of(j * chunk, chunk) + c * sub, sub)
        gw_ref[:, cols] += dot(zt, q_sc[:, c * sub:(c + 1) * sub])
    dz_ref[...] += contract_cols(q_sc[...], w_ref[:, pl.ds(pl.multiple_of(j * chunk, chunk), chunk)])


def pass2(logits, z_all, w_loc, lse_rows, wt_rows, tgt_rows, dz_in, part, parts, chunk=1024, sub=512, tile=1024):
    tokens, width = z_all.shape
    vl = w_loc.shape[1]
    vp = vl // parts
    nj = vp // chunk
    first = dz_in is None
    row_spec = pl.BlockSpec((tile // 128, 128), lambda i, j: (i, 0))
    dz_spec = pl.BlockSpec((tile, width), lambda i, j: (i, 0))
    return pl.pallas_call(
        functools.partial(pass2_kernel, chunk=chunk, sub=sub, vocab_local=vl, part_base=part * vp, first=first),
        grid=(tokens // tile, nj),
        out_shape=(jax.ShapeDtypeStruct((width, vp), F32), jax.ShapeDtypeStruct((tokens, width), F32)),
        in_specs=[
            pl.BlockSpec((tile, chunk), lambda i, j: (i, part * nj + j)),
            dz_spec,
            pl.BlockSpec((width, vp), lambda i, j: (0, part)),
            row_spec, row_spec, row_spec,
        ] + ([] if first else [dz_spec]),
        out_specs=(pl.BlockSpec((width, vp), lambda i, j: (0, 0)), dz_spec),
        scratch_shapes=[
            pltpu.VMEM((width, tile), BF16), pltpu.VMEM((tile, chunk), BF16),
            pltpu.VMEM((tile, 128), F32), pltpu.VMEM((tile, 128), F32), pltpu.VMEM((tile, 128), jnp.int32),
        ],
        compiler_params=params('arbitrary', 'arbitrary'),
        cost_estimate=pl.CostEstimate(flops=4 * tokens * width * vp, bytes_accessed=4 * tokens * vp, transcendentals=tokens * vp),
        name=f'head_pass2_{part}',
    )(logits, z_all, w_loc, lse_rows, wt_rows, tgt_rows, *([] if first else [dz_in]))


def swap(x, k):
    return lax.ppermute(x, AXIS, [(i, i ^ k) for i in range(NDEV)])


def pick(x, index, axis=0):
    return lax.dynamic_index_in_dim(x, index, axis, keepdims=False)


def pair_then_chips(partial, me):
    core, chip = me % 2, me // 2
    halves = partial.reshape((4, 2) + partial.shape[1:])
    got = swap(pick(halves, 1 - core, 1), 1)
    mine = pick(halves, core, 1) + got
    total = pick(mine, chip)
    for k in (1, 2, 3):
        total = total + swap(pick(mine, chip ^ k).astype(BF16), 2 * k).astype(F32)
    return total


def solution(mesh):
    def device_step(hidden, w_gate, w_up, w_down, w_out, targets, loss_mask):
        layers, tok, width = hidden.shape
        top = layers - 1
        vocab = w_out.shape[1]
        vl = vocab // NDEV
        tokens = tok * NDEV
        me = lax.axis_index(AXIS)
        order = jnp.bitwise_xor(jnp.arange(NDEV), me)

        def gather(x):
            return lax.all_gather(x, AXIS, axis=1, tiled=True)

        wg5, wu5, wd5 = gather(w_gate[top:]), gather(w_up[top:]), gather(w_down[top:])
        w_loc = lax.all_to_all(w_out, AXIS, 1, 0, tiled=True)
        labels = small_gather(jnp.stack([targets.reshape(tok // 128, 128), loss_mask.reshape(tok // 128, 128)]), 1)
        labels = labels[order]
        tgt_rows = labels[:, 0].reshape(tokens // 128, 128)
        mask_rows = labels[:, 1].reshape(tokens // 128, 128).astype(F32)
        wt_rows = mask_rows / jnp.sum(mask_rows)

        t_top, z = top_forward(hidden, top, wg5, wu5, wd5, 0)
        z_all = lax.all_gather(z, AXIS, axis=0, tiled=True)

        wgr, wur, wdr, z_all = lax.optimization_barrier((w_gate[:top], w_up[:top], w_down[:top], z_all))
        wgr, wur, wdr = gather(wgr), gather(wur), gather(wdr)

        logits, stats = pass1(z_all, w_loc, tgt_rows)
        stats = small_gather(stats, 2)[order]
        lse_dev = stats[:, 0]
        lse_max = jnp.max(lse_dev, axis=0)
        lse = lse_max + jnp.log(jnp.sum(jnp.exp(lse_dev - lse_max), axis=0))
        mean_loss = jnp.sum(wt_rows * (lse - jnp.sum(stats[:, 1], axis=0)))

        parts = 2
        vp = vl // parts
        dz = None
        pieces = []
        for part in range(parts):
            gw, dz = pass2(logits, z_all, w_loc, lse, wt_rows, tgt_rows, dz, part, parts)
            gw = gw.reshape(NDEV, width // NDEV, vp)
            own = pick(gw, me)
            pieces.append([own] + [swap(pick(gw, me ^ k).astype(BF16), k) for k in range(1, NDEV)])
        grad_out = jnp.zeros((width // NDEV, vocab), F32)
        for part in range(parts):
            for k in range(NDEV):
                grad_out = lax.dynamic_update_slice(grad_out, pieces[part][k].astype(F32), (0, (me ^ k) * vl + part * vp))

        dz_own = pair_then_chips(dz.reshape(NDEV, tok, width), me)
        g = norm_grad(t_top.astype(F32), dz_own)

        gates, ups, downs, grad_hidden = blocks_backward(hidden, g, (wg5, wu5, wd5), (wgr, wur, wdr))
        return gates, ups, downs, grad_out, grad_hidden, mean_loss

    stacked = P(None, AXIS, None)
    row = P(AXIS, None)
    return jax.shard_map(device_step, mesh=mesh, in_specs=(stacked, stacked, stacked, stacked, row, P(AXIS), P(AXIS)), out_specs=(stacked, stacked, stacked, row, row, P()), check_vma=False)
```
